256 devices in a mesh: row: 16 (over z_hi, y, core), col: 16 (over x, z_lo).
Axes of the slice: x: 4, y: 4, z: 8 (z_hi: 2, z_lo: 4; z = z_hi * 4 + z_lo), core: 2. Of those that a mesh axis runs over, the one named last changes fastest.
Arguments:
- series: float32 [16384, 2048], P(('row', 'col'))
- lengths: int32 [16384], P(('row', 'col')), may hold values from 512 to 2048
- starts: int32 [16384], P(('row', 'col')), may hold values from 0 to 1536, as said below
Outputs:
- correlation: float32 [16384, 16384], P('row', 'col')
The draws below stay inside these ranges and needn't reach their ends.
Inputs may be any that keep to these rules, and one draw needn't show every extreme that they name: starts[s] + lengths[s] <= 2048 for every series.
All inputs are finite; a program needn't handle non-finite values.
Results may differ from the reference program's by a relative error of at most 0.0012.
Values may be sent and summed in bfloat16 or wider, within the bound.
A program may use at most 64 MiB of HBM per device.

```python
import math
import jax
import jax.numpy as jnp
from jax import lax

STEPS = 2048
SERIES = 16384
N_ROW = 16


factor_total = 24


def draw_series(key, part):
    subkeys = jax.random.split(jax.random.fold_in(key, 11), 6)
    factors = jax.random.normal(subkeys[0], (factor_total, STEPS), jnp.float32)
    loadings = jax.random.normal(subkeys[1], (SERIES, factor_total), jnp.float32)
    common = jnp.dot(loadings, factors) / math.sqrt(factor_total)
    column_scale = jnp.exp(jax.random.uniform(subkeys[2], (1, STEPS), jnp.float32, 0.0, math.log(3.0)))
    noise = jax.random.normal(subkeys[3], (SERIES, STEPS), jnp.float32)
    level = jax.random.uniform(subkeys[4], (SERIES, 1), jnp.float32, -3.0, 3.0)
    row_scale = jnp.exp(jax.random.uniform(subkeys[5], (SERIES, 1), jnp.float32, 0.0, math.log(10.0)))
    values = level + row_scale * column_scale * (common + 0.7 * noise)
    return values.astype(jnp.float32)


def windows(key):
    subkeys = jax.random.split(jax.random.fold_in(key, 7), 4)
    lengths = jax.random.randint(subkeys[0], (SERIES,), STEPS // 4, STEPS + 1, jnp.int32)
    longest = jax.random.randint(subkeys[1], (), 0, SERIES // 2, jnp.int32)
    shortest = SERIES // 2 + jax.random.randint(subkeys[2], (), 0, SERIES // 2, jnp.int32)
    lengths = lengths.at[longest].set(STEPS).at[shortest].set(STEPS // 4)
    raw_bits = jax.random.randint(subkeys[3], (SERIES,), 0, 1 << 30, jnp.int32)
    starts = raw_bits % (STEPS - lengths + 1)
    starts = starts.at[shortest].set(STEPS - STEPS // 4)
    return (lengths, starts)


def draw_lengths(key, part):
    return windows(key)[0]


def draw_starts(key, part):
    return windows(key)[1]


def setup_inputs(seed: int = 0) -> dict:
    key_of = jax.random.split(jax.random.key(seed), 4)
    return {
        "series": draw_series(jax.random.fold_in(key_of[3], 71), 0),
        "lengths": draw_lengths(jax.random.fold_in(key_of[3], 71), 0),
        "starts": draw_starts(jax.random.fold_in(key_of[3], 71), 0),
    }


def normalize(series, lengths, starts):
    positions = jnp.arange(series.shape[1], dtype=jnp.int32)[None, :]
    inside = ((positions >= starts[:, None]) & (positions < (starts + lengths)[:, None])).astype(jnp.float32)
    valid_count = lengths.astype(jnp.float32)[:, None]
    average = lax.optimization_barrier(jnp.sum(inside * series, axis=1, keepdims=True)) / valid_count
    centered = inside * (series - average)
    variance = lax.optimization_barrier(jnp.sum(centered * centered, axis=1, keepdims=True)) / valid_count
    return (centered / jnp.sqrt(valid_count * (variance + 1e-06))).astype(jnp.bfloat16)

def reference(series, lengths, starts):
    normed = normalize(series, lengths, starts)
    block_rows = SERIES // N_ROW
    blocks = normed.reshape(N_ROW, block_rows, STEPS)

    def one_block(rows_block):
        return lax.dot_general(rows_block, normed, (((1,), (1,)), ((), ())), preferred_element_type=jnp.float32)
    return lax.map(one_block, blocks).reshape(SERIES, SERIES)
```

```python
import jax
import jax.numpy as jnp
from jax import lax
from jax.experimental import pallas as pl
from jax.experimental.pallas import tpu as pltpu
from jax.sharding import PartitionSpec as P

MESH = pl.DeviceIdType.MESH


def normalize(series, lengths, starts):
    positions = jnp.arange(series.shape[1], dtype=jnp.int32)[None, :]
    inside = ((positions >= starts[:, None]) & (positions < (starts + lengths)[:, None])).astype(
        jnp.float32
    )
    valid_count = lengths.astype(jnp.float32)[:, None]
    average = jnp.sum(inside * series, axis=1, keepdims=True) / valid_count
    centered = inside * (series - average)
    variance = jnp.sum(centered * centered, axis=1, keepdims=True) / valid_count
    return (centered / jnp.sqrt(valid_count * (variance + 1e-06))).astype(jnp.bfloat16)


def exchange(own, out, rows, cols, send_sem, row_sem, col_sem):
    row, col = lax.axis_index("row"), lax.axis_index("col")
    half, y, core = row // 8, (row // 2) % 4, row % 2
    x, z = col // 4, col % 4
    right, left = (x + 1) % 4, (x + 3) % 4
    up, down = (y + 1) % 4, (y + 3) % 4

    def at_col(x_to, z_to):
        return (row, x_to * 4 + z_to)

    def at_y(y_to):
        return (half * 8 + y_to * 2 + core, col)

    sibling = (row + 1 - 2 * core, col)
    line = [at_col(x, (z + s) % 4) for s in (1, 2, 3)]
    sides = [at_col(right, z), at_col(left, z)]
    ring = [at_y(up), at_y(down)]
    taker = 1 - x % 2
    targets = [(h * 8 + z * 2 + taker, row) for h in (0, 1)]
    first, second = 1 - core, 3 - core
    sources = [(col, first * 4 + y), (col, second * 4 + y)]

    barrier = pltpu.get_barrier_semaphore()
    for device in line + sides + ring + [sibling] + sources:
        pl.semaphore_signal(barrier, inc=1, device_id=device, device_id_type=MESH)
    pl.semaphore_wait(barrier, 10)

    sent = []

    def send(src, dst, sem, device):
        copy = pltpu.make_async_remote_copy(
            src_ref=src,
            dst_ref=dst,
            send_sem=send_sem.at[len(sent)],
            recv_sem=sem,
            device_id=device,
            device_id_type=MESH,
        )
        copy.start()
        sent.append(copy)

    def send_row(slot, device, src=None):
        send(rows.at[slot] if src is None else src, rows.at[slot], row_sem.at[slot], device)

    def send_col(slot, device, src=None):
        send(cols.at[slot] if src is None else src, cols.at[slot], col_sem.at[slot], device)

    def wait(buffer, sem, slot):
        pltpu.make_async_remote_copy(
            src_ref=buffer.at[slot],
            dst_ref=buffer.at[slot],
            send_sem=send_sem.at[0],
            recv_sem=sem.at[slot],
            device_id=sibling,
            device_id_type=MESH,
        ).wait_recv()

    def wait_row(slot):
        wait(rows, row_sem, slot)

    def wait_col(slot):
        wait(cols, col_sem, slot)

    def row_slot(x_of, z_back):
        return x_of * 4 + (z + 4 - z_back) % 4

    for target in targets:
        send_col(col, target, own)
    for side in sides:
        send_row(col, side, own)
    for device in line:
        send_row(col, device, own)
    rows[col] = own[...]

    def pass_line(s):
        slot = row_slot(x, s)
        wait_row(slot)
        for side in sides:
            send_row(slot, side)

    def relay(x_from, side, s):
        slot = row_slot(x_from, s)
        wait_row(slot)
        send_row(slot, side)

    def col_slot(x_of, y_of):
        return x_of * 4 + y_of

    pass_line(1)
    for x_of in (first, second):
        slot = col_slot(x_of, y)
        wait_col(slot)
        for device in ring:
            send_col(slot, device)
        send_col(slot, sibling)
    relay(left, sides[0], 0)
    relay(right, sides[1], 1)
    pass_line(2)
    for x_of, y_of, device in ((first, down, ring[0]), (second, up, ring[1])):
        slot = col_slot(x_of, y_of)
        wait_col(slot)
        send_col(slot, device)
        send_col(slot, sibling)
    pass_line(3)
    for x_of, y_of in ((first, up), (second, down)):
        slot = col_slot(x_of, y_of)
        wait_col(slot)
        send_col(slot, sibling)
    relay(left, sides[0], 2)
    for x_of in (first, second):
        slot = col_slot(x_of, (y + 2) % 4)
        wait_col(slot)
        send_col(slot, sibling)
    relay(right, sides[1], 3)
    for x_of in (core, core + 2):
        for y_of in range(4):
            wait_col(col_slot(x_of, y_of))

    steps = rows.shape[2]

    def product(group):
        left_rows = rows[pl.ds(group * 4, 4)].reshape(256, steps)

        def tile(n, carry):
            right_rows = cols[pl.ds(n * 4, 4)].reshape(256, steps)
            block = lax.dot_general(
                left_rows,
                right_rows,
                (((1,), (1,)), ((), ())),
                preferred_element_type=jnp.float32,
            )
            out[pl.ds(group * 256, 256), pl.ds(pl.multiple_of(n * 256, 256), 256)] = block
            return carry

        lax.fori_loop(0, 4, tile, 0)

    far = (x + 2) % 4

    product(x)
    wait_row(row_slot(left, 1))
    wait_row(row_slot(left, 3))
    product(left)
    wait_row(row_slot(right, 0))
    wait_row(row_slot(right, 2))
    product(right)
    for s in range(4):
        wait_row(row_slot(far, s))
    product(far)
    for copy in sent:
        copy.wait_send()


def on_device(series, lengths, starts):
    normed = normalize(series, lengths, starts)
    pieces, steps = normed.shape
    shape = (16, pieces, steps)
    return pl.pallas_call(
        exchange,
        out_shape=jax.ShapeDtypeStruct((1024, 1024), jnp.float32),
        in_specs=[pl.BlockSpec(memory_space=pltpu.VMEM)],
        out_specs=pl.BlockSpec(memory_space=pltpu.VMEM),
        scratch_shapes=[
            pltpu.VMEM(shape, jnp.bfloat16),
            pltpu.VMEM(shape, jnp.bfloat16),
            pltpu.SemaphoreType.DMA((31,)),
            pltpu.SemaphoreType.DMA((16,)),
            pltpu.SemaphoreType.DMA((16,)),
        ],
        compiler_params=pltpu.CompilerParams(
            collective_id=0, has_side_effects=True, vmem_limit_bytes=40 * 1024 * 1024
        ),
        name="exchange",
    )(normed)


def solution(mesh):
    placed = (P(("row", "col"), None), P(("row", "col")), P(("row", "col")))
    return jax.shard_map(
        on_device, mesh=mesh, in_specs=placed, out_specs=P("row", "col"), check_vma=False
    )
```

```python
import functools

import jax
import jax.numpy as jnp
from jax import lax
from jax.experimental import pallas as pl
from jax.experimental.pallas import tpu as pltpu
from jax.sharding import PartitionSpec as P

MESH = pl.DeviceIdType.MESH


def normalize(series, lengths, starts, normed):
    count, steps = series.shape
    diagonal = lax.broadcasted_iota(jnp.int32, (count, count), 0) == lax.broadcasted_iota(
        jnp.int32, (count, count), 1
    )

    def column(values):
        spread = jnp.where(diagonal, jnp.broadcast_to(values[...], (count, count)), 0)
        return jnp.sum(spread, axis=1, keepdims=True)

    valid, first = column(lengths), column(starts)
    positions = lax.broadcasted_iota(jnp.int32, (count, steps), 1)
    inside = ((positions >= first) & (positions < first + valid)).astype(jnp.float32)
    valid_count = valid.astype(jnp.float32)
    average = jnp.sum(inside * series[...], axis=1, keepdims=True) / valid_count
    centered = inside * (series[...] - average)
    variance = jnp.sum(centered * centered, axis=1, keepdims=True) / valid_count
    normed[...] = (centered / jnp.sqrt(valid_count * (variance + 1e-06))).astype(jnp.bfloat16)


PARTS = 2
COPIES = 120
FIRST = ["o", "x", "c"]
ORDER = (
    ("l1", "l2.m", "p", "h0", "l3.m", "l2.e", "h1", "f", "l3.e", "h2", "y", "h3", "v", "A", "B")
    + ("w", "C", "D")
)


def exchange(own, out, rows, cols, passing, send_sem, row_sem, col_sem, passing_sem):
    row, col = lax.axis_index("row"), lax.axis_index("col")
    half, y, core = row // 8, (row // 2) % 4, row % 2
    x, z = col // 4, col % 4
    right, left = (x + 1) % 4, (x + 3) % 4
    up, down = (y + 1) % 4, (y + 3) % 4

    def at_col(x_to, z_to):
        return (row, x_to * 4 + z_to)

    def at_y(y_to):
        return (half * 8 + y_to * 2 + core, col)

    sibling = (row + 1 - 2 * core, col)
    heights = [z, z + 1 - 2 * (z % 2), 2 - z // 2, 3 - 3 * (z // 2)]
    middle = z * (3 - z) // 2
    partner = at_col(x, heights[1])
    across = at_col(x, (3 - z) % 4)
    sides = [at_col(right, z), at_col(left, z)]
    ring = [at_y(up), at_y(down)]
    shift = 2 * (x % 2) + z // 2
    carrier = at_y((y + shift) % 4)
    moves = (shift + 3) // 4
    source = at_y((y + 4 - shift) % 4)
    theirs = half * 8 + ((y + 4 - shift) % 4) * 2 + core
    targets = [(h * 8 + y * 2 + 1 - z % 2, theirs) for h in (0, 1)]
    origin = (col // 2) % 4

    def places(y_of, height):
        turn = (y_of + 4 - origin) % 4
        near = turn // 2 * 4 + turn % 2 * 2 + height
        return near, near + 8

    carriers = [
        (col // 8 * 8 + y * 2 + col % 2, place) for place in places(y, 1 - core)
    ]

    barrier = pltpu.get_barrier_semaphore()

    def greet(device):
        pl.semaphore_signal(barrier, inc=1, device_id=device, device_id_type=MESH)

    for device in [partner, sibling] + sides + ring + carriers:
        greet(device)
    pl.when(middle == 1)(functools.partial(greet, across))
    pl.when(moves == 1)(functools.partial(greet, source))
    pl.semaphore_wait(barrier, 8 + middle + moves)

    sent = []

    def both(a, b):
        return b if a is None else a if b is None else a * b

    def send(src, dst, sem, device, when=None):
        copy = pltpu.make_async_remote_copy(
            src_ref=src,
            dst_ref=dst,
            send_sem=send_sem.at[len(sent)],
            recv_sem=sem,
            device_id=device,
            device_id_type=MESH,
        )
        if when is None:
            copy.start()
        else:
            pl.when(when == 1)(copy.start)
        sent.append((copy, when))

    def mine(part):
        return own.at[pl.ds(part * (64 // PARTS), 64 // PARTS)]

    def send_row(slot, part, device, src=None, when=None):
        i = slot * PARTS + part
        send(rows.at[i] if src is None else src, rows.at[i], row_sem.at[i], device, when)

    def send_col(slot, part, device, when=None):
        i = slot * PARTS + part
        send(cols.at[i], cols.at[i], col_sem.at[i], device, when)

    def wait(buffer, sem, i, when=None):
        copy = pltpu.make_async_remote_copy(
            src_ref=buffer.at[i],
            dst_ref=buffer.at[i],
            send_sem=send_sem.at[0],
            recv_sem=sem.at[i],
            device_id=sibling,
            device_id_type=MESH,
        )
        if when is None:
            copy.wait_recv()
        else:
            pl.when(when == 1)(copy.wait_recv)

    def wait_row(slot, part, when=None):
        wait(rows, row_sem, slot * PARTS + part, when)

    def wait_col(slot, part, when=None):
        wait(cols, col_sem, slot * PARTS + part, when)

    def carry(src, part, when):
        i = col * PARTS + part
        for target in targets:
            send(src, cols.at[i], col_sem.at[i], target, when)

    def start(name):
        for part in range(PARTS):
            if name == "x":
                for side in sides:
                    send_row(col, part, side, mine(part))
            elif name == "c":
                send(mine(part), passing.at[part], passing_sem.at[part], carrier, moves)
                carry(mine(part), part, 1 - moves)
            else:
                send_row(col, part, partner, mine(part))
                send_row(col, part, across, mine(part), middle)

    for name in FIRST:
        start(name)
    rows[pl.ds(col * PARTS, PARTS)] = own[...].reshape(PARTS, 64 // PARTS, own.shape[1])

    def step(name):
        kind, k = name[0], int(name[1:2].strip(".") or 0)
        on = None if "." not in name else middle if name[-1] == "m" else 1 - middle
        for part in range(PARTS):
            onward = part < PARTS // 2
            if kind == "l":
                slot = x * 4 + heights[k]
                wait_row(slot, part, on)
                if "e" not in name:
                    send_row(slot, part, across if k == 1 else partner, None, middle)
                for side in sides:
                    send_row(slot, part, side, None, on)
            elif kind == "h":
                slot = (left if onward else right) * 4 + heights[k]
                wait_row(slot, part, on)
                send_row(slot, part, sides[0] if onward else sides[1], None, on)
            elif kind == "p":
                wait(passing, passing_sem, part, both(moves, on))
                carry(passing.at[part], part, both(moves, on))
            else:
                if kind == "f":
                    y_of, onto = y, ring
                elif kind == "y":
                    y_of, onto = (down, ring[:1]) if onward else (up, ring[1:])
                elif kind == "v":
                    y_of, onto = up if onward else down, []
                else:
                    y_of, onto = (y + 2) % 4, []
                for slot in places(y_of, 1 - core):
                    wait_col(slot, part, on)
                    for device in onto:
                        send_col(slot, part, device, on)
                    send_col(slot, part, sibling, on)

    steps = rows.shape[2]

    def tile(group, groups, y_of):
        count = 4 * groups * PARTS
        left_rows = rows[pl.ds(group * 4 * PARTS, count)].reshape(groups * 256, steps)
        near, beyond = places(y_of, 0)
        right_rows = jnp.concatenate(
            [cols[pl.ds(place * PARTS, 2 * PARTS)].reshape(128, steps) for place in (near, beyond)],
            axis=0,
        )
        block = lax.dot_general(
            left_rows, right_rows, (((1,), (1,)), ((), ())), preferred_element_type=jnp.float32
        )
        for k, place in enumerate((near, beyond)):
            at = pl.multiple_of(place * 64, 128)
            out[pl.ds(group * 256, groups * 256), pl.ds(at, 128)] = block[:, k * 128 : k * 128 + 128]

    def wait_siblings(y_of):
        for slot in places(y_of, core):
            for part in range(PARTS):
                wait_col(slot, part)

    def loop(count, body):
        def run(i, carry):
            body(i)
            return carry

        lax.fori_loop(0, count, run, 0)

    def multiply(name):
        if name == "A":
            wait_siblings(y)
            tile(x, 1, y)
        elif name == "B":
            wait_siblings(down)
            wait_siblings(up)
            for height in range(4):
                for part in range(PARTS):
                    wait_row((right if part < PARTS // 2 else left) * 4 + height, part)

            def body(i):
                j, k = (i + 1) // 3, (i + 1) % 3
                tile((x + j + j // 2) % 4, 1, (y + k + k // 2) % 4)

            loop(8, body)
        elif name == "C":
            for height in range(4):
                for part in range(PARTS):
                    wait_row((x + 2) % 4 * 4 + height, part)
            loop(3, lambda k: tile((x + 2) % 4, 1, (y + k + k // 2) % 4))
        else:
            wait_siblings((y + 2) % 4)
            loop(2, lambda i: tile(2 * i, 2, (y + 2) % 4))

    for name in ORDER:
        if name.isupper():
            multiply(name)
        else:
            step(name)
    for copy, when in sent:
        if when is None:
            copy.wait_send()
        else:
            pl.when(when == 1)(copy.wait_send)


def on_device(series, lengths, starts):
    pieces, steps = series.shape
    normed = pl.pallas_call(
        normalize,
        out_shape=jax.ShapeDtypeStruct(series.shape, jnp.bfloat16),
        in_specs=[pl.BlockSpec(memory_space=pltpu.VMEM)] * 3,
        out_specs=pl.BlockSpec(memory_space=pltpu.VMEM),
        compiler_params=pltpu.CompilerParams(vmem_limit_bytes=16 * 1024 * 1024),
        name="normalize",
    )(series, lengths.reshape(1, pieces), starts.reshape(1, pieces))
    part = pieces // PARTS
    shape = (16 * PARTS, part, steps)
    return pl.pallas_call(
        exchange,
        out_shape=jax.ShapeDtypeStruct((1024, 1024), jnp.float32),
        in_specs=[pl.BlockSpec(memory_space=pltpu.VMEM)],
        out_specs=pl.BlockSpec(memory_space=pltpu.VMEM),
        scratch_shapes=[
            pltpu.VMEM(shape, jnp.bfloat16),
            pltpu.VMEM(shape, jnp.bfloat16),
            pltpu.VMEM((PARTS, part, steps), jnp.bfloat16),
            pltpu.SemaphoreType.DMA((COPIES,)),
            pltpu.SemaphoreType.DMA((16 * PARTS,)),
            pltpu.SemaphoreType.DMA((16 * PARTS,)),
            pltpu.SemaphoreType.DMA((PARTS,)),
        ],
        compiler_params=pltpu.CompilerParams(
            collective_id=0, has_side_effects=True, vmem_limit_bytes=40 * 1024 * 1024
        ),
        name="exchange",
    )(normed)


def solution(mesh):
    placed = (P(("row", "col"), None), P(("row", "col")), P(("row", "col")))
    return jax.shard_map(
        on_device, mesh=mesh, in_specs=placed, out_specs=P("row", "col"), check_vma=False
    )
```

```python
import functools

import jax
import jax.numpy as jnp
from jax import lax
from jax.experimental import pallas as pl
from jax.experimental.pallas import tpu as pltpu
from jax.sharding import PartitionSpec as P

MESH = pl.DeviceIdType.MESH


def normalize(series, lengths, starts):
    count, steps = series.shape
    diagonal = lax.broadcasted_iota(jnp.int32, (count, count), 0) == lax.broadcasted_iota(
        jnp.int32, (count, count), 1
    )

    def column(values):
        spread = jnp.where(diagonal, jnp.broadcast_to(values[...], (count, count)), 0)
        return jnp.sum(spread, axis=1, keepdims=True)

    valid, first = column(lengths), column(starts)
    positions = lax.broadcasted_iota(jnp.int32, (count, steps), 1)
    inside = ((positions >= first) & (positions < first + valid)).astype(jnp.float32)
    valid_count = valid.astype(jnp.float32)
    average = jnp.sum(inside * series[...], axis=1, keepdims=True) / valid_count
    centered = inside * (series[...] - average)
    variance = jnp.sum(centered * centered, axis=1, keepdims=True) / valid_count
    return (centered / jnp.sqrt(valid_count * (variance + 1e-06))).astype(jnp.bfloat16)


PARTS = 2
COPIES = 140
SHORT = 1
FIRST = ["o", "x", "c"]
ORDER = (
    ("p", "l1", "l2.m", "h0", "h1", "f", "l3.m", "l2.e", "l3.e", "h2", "y", "q", "v", "w", "h3")
    + ("A", "B", "C", "D")
)


def exchange(series_in, lengths_in, starts_in, out, *scratch):
    series, lengths, starts, own, rows, cols, passing = scratch[:7]
    send_sem, row_sem, col_sem, passing_sem, in_sem = scratch[7:]
    row, col = lax.axis_index("row"), lax.axis_index("col")
    half, y, core = row // 8, (row // 2) % 4, row % 2
    x, z = col // 4, col % 4
    right, left = (x + 1) % 4, (x + 3) % 4
    up, down = (y + 1) % 4, (y + 3) % 4

    def at_col(x_to, z_to):
        return (row, x_to * 4 + z_to)

    def at_y(y_to):
        return (half * 8 + y_to * 2 + core, col)

    sibling = (row + 1 - 2 * core, col)
    heights = [z, z + 1 - 2 * (z % 2), 2 - z // 2, 3 - 3 * (z // 2)]
    middle = z * (3 - z) // 2
    partner = at_col(x, heights[1])
    across = at_col(x, (3 - z) % 4)
    sides = [at_col(right, z), at_col(left, z)]
    ring = [at_y(up), at_y(down)]
    shift = 2 * (x % 2) + z // 2
    carrier = at_y((y + shift) % 4)
    moves = (shift + 3) // 4
    source = at_y((y + 4 - shift) % 4)
    theirs = half * 8 + ((y + 4 - shift) % 4) * 2 + core
    targets = [(h * 8 + y * 2 + 1 - z % 2, theirs) for h in (0, 1)]
    origin = (col // 2) % 4

    def places(y_of, height):
        turn = (y_of + 4 - origin) % 4
        near = turn // 2 * 4 + turn % 2 * 2 + height
        return near, near + 8

    carriers = [
        (col // 8 * 8 + y * 2 + col % 2, place) for place in places(y, 1 - core)
    ]

    loads = [
        pltpu.make_async_copy(src, dst, in_sem.at[i])
        for i, (src, dst) in enumerate(
            ((series_in, series), (lengths_in, lengths), (starts_in, starts))
        )
    ]
    for load in loads:
        load.start()
    barrier = pltpu.get_barrier_semaphore()

    def greet(device):
        pl.semaphore_signal(barrier, inc=1, device_id=device, device_id_type=MESH)

    for device in [partner, sibling] + sides + ring + carriers:
        greet(device)
    pl.when(middle == 1)(functools.partial(greet, across))
    pl.when(moves == 1)(functools.partial(greet, source))
    for load in loads:
        load.wait()
    normed = normalize(series, lengths, starts)
    own[...] = normed
    rows[pl.ds(col * PARTS, PARTS)] = normed.reshape(PARTS, 64 // PARTS, own.shape[1])
    pl.semaphore_wait(barrier, 8 + middle + moves)

    sent = []

    def both(a, b):
        return b if a is None else a if b is None else a * b

    def send(src, dst, sem, device, when=None):
        copy = pltpu.make_async_remote_copy(
            src_ref=src,
            dst_ref=dst,
            send_sem=send_sem.at[len(sent)],
            recv_sem=sem,
            device_id=device,
            device_id_type=MESH,
        )
        if when is None:
            copy.start()
        else:
            pl.when(when == 1)(copy.start)
        sent.append((copy, when))

    def mine(part):
        return own.at[pl.ds(part * (64 // PARTS), 64 // PARTS)]

    def send_row(slot, part, device, src=None, when=None):
        i = slot * PARTS + part
        send(rows.at[i] if src is None else src, rows.at[i], row_sem.at[i], device, when)

    def send_col(slot, part, device, when=None):
        i = slot * PARTS + part
        send(cols.at[i], cols.at[i], col_sem.at[i], device, when)

    def wait(buffer, sem, i, when=None):
        copy = pltpu.make_async_remote_copy(
            src_ref=buffer.at[i],
            dst_ref=buffer.at[i],
            send_sem=send_sem.at[0],
            recv_sem=sem.at[i],
            device_id=sibling,
            device_id_type=MESH,
        )
        if when is None:
            copy.wait_recv()
        else:
            pl.when(when == 1)(copy.wait_recv)

    def wait_row(slot, part, when=None):
        wait(rows, row_sem, slot * PARTS + part, when)

    def wait_col(slot, part, when=None):
        wait(cols, col_sem, slot * PARTS + part, when)

    def carry(src, part, when):
        i = col * PARTS + part
        for target in targets:
            send(src, cols.at[i], col_sem.at[i], target, when)

    def start(name):
        for part in range(PARTS):
            if name == "x":
                for side in sides:
                    send_row(col, part, side, mine(part))
            elif name == "c":
                send(mine(part), passing.at[part], passing_sem.at[part], carrier, moves)
                carry(mine(part), part, 1 - moves)
            else:
                send_row(col, part, partner, mine(part))
                send_row(col, part, across, mine(part), middle)

    for name in FIRST:
        start(name)

    def step(name):
        kind, k = name[0], int(name[1:2].strip(".") or 0)
        on = None if "." not in name else middle if name[-1] == "m" else 1 - middle
        for part in range(PARTS):
            onward = part < PARTS // 2
            if kind == "l":
                slot = x * 4 + heights[k]
                wait_row(slot, part, on)
                if "e" not in name:
                    send_row(slot, part, across if k == 1 else partner, None, middle)
                one_way = k == 1 or (k == 2 and SHORT and "m" in name)
                for side in (sides[:1] if onward else sides[1:]) if one_way else sides:
                    send_row(slot, part, side, None, on)
            elif kind == "q":
                slot = (right if onward else left) * 4 + z
                wait_row(slot, part, on)
                send_row(slot, part, partner, None, on)
                if SHORT:
                    send_row(slot, part, across, None, middle if on is None or "m" in name else 0 * z)
            elif kind == "h":
                slot = (left if onward else right) * 4 + heights[k]
                wait_row(slot, part, on)
                send_row(slot, part, sides[0] if onward else sides[1], None, on)
            elif kind == "p":
                wait(passing, passing_sem, part, both(moves, on))
                carry(passing.at[part], part, both(moves, on))
            else:
                if kind == "f":
                    y_of, onto = y, ring
                elif kind == "y":
                    y_of, onto = (down, ring[:1]) if onward else (up, ring[1:])
                elif kind == "v":
                    y_of, onto = up if onward else down, []
                else:
                    y_of, onto = (y + 2) % 4, []
                for slot in places(y_of, 1 - core):
                    wait_col(slot, part, on)
                    for device in onto:
                        send_col(slot, part, device, on)
                    send_col(slot, part, sibling, on)

    steps = rows.shape[2]

    def tile(group, groups, y_of):
        count = 4 * groups * PARTS
        left_rows = rows[pl.ds(group * 4 * PARTS, count)].reshape(groups * 256, steps)
        near, beyond = places(y_of, 0)
        right_rows = jnp.concatenate(
            [cols[pl.ds(place * PARTS, 2 * PARTS)].reshape(128, steps) for place in (near, beyond)],
            axis=0,
        )
        block = lax.dot_general(
            left_rows, right_rows, (((1,), (1,)), ((), ())), preferred_element_type=jnp.float32
        )
        for k, place in enumerate((near, beyond)):
            at = pl.multiple_of(place * 64, 128)
            out[pl.ds(group * 256, groups * 256), pl.ds(at, 128)] = block[:, k * 128 : k * 128 + 128]

    def wait_siblings(y_of):
        for slot in places(y_of, core):
            for part in range(PARTS):
                wait_col(slot, part)

    def loop(count, body):
        def run(i, carry):
            body(i)
            return carry

        lax.fori_loop(0, count, run, 0)

    def multiply(name):
        if name == "A":
            wait_siblings(y)
            tile(x, 1, y)
        elif name == "B":
            wait_siblings(down)
            wait_siblings(up)
            for height in heights[1:]:
                for part in range(PARTS):
                    wait_row((right if part < PARTS // 2 else left) * 4 + height, part)

            def body(i):
                j, k = (i + 1) // 3, (i + 1) % 3
                tile((x + j + j // 2) % 4, 1, (y + k + k // 2) % 4)

            loop(8, body)
        elif name == "C":
            for height in range(4):
                for part in range(PARTS):
                    wait_row((x + 2) % 4 * 4 + height, part)
            loop(3, lambda k: tile((x + 2) % 4, 1, (y + k + k // 2) % 4))
        else:
            wait_siblings((y + 2) % 4)
            loop(2, lambda i: tile(2 * i, 2, (y + 2) % 4))

    for name in ORDER:
        if name.isupper():
            multiply(name)
        else:
            step(name)
    for copy, when in sent:
        if when is None:
            copy.wait_send()
        else:
            pl.when(when == 1)(copy.wait_send)


def on_device(series, lengths, starts):
    pieces, steps = series.shape
    part = pieces // PARTS
    shape = (16 * PARTS, part, steps)
    return pl.pallas_call(
        exchange,
        out_shape=jax.ShapeDtypeStruct((1024, 1024), jnp.float32),
        in_specs=[pl.BlockSpec(memory_space=pltpu.HBM)] * 3,
        out_specs=pl.BlockSpec(memory_space=pltpu.VMEM),
        scratch_shapes=[
            pltpu.VMEM((pieces, steps), jnp.float32),
            pltpu.VMEM((1, pieces), jnp.int32),
            pltpu.VMEM((1, pieces), jnp.int32),
            pltpu.VMEM((pieces, steps), jnp.bfloat16),
            pltpu.VMEM(shape, jnp.bfloat16),
            pltpu.VMEM(shape, jnp.bfloat16),
            pltpu.VMEM((PARTS, part, steps), jnp.bfloat16),
            pltpu.SemaphoreType.DMA((COPIES,)),
            pltpu.SemaphoreType.DMA((16 * PARTS,)),
            pltpu.SemaphoreType.DMA((16 * PARTS,)),
            pltpu.SemaphoreType.DMA((PARTS,)),
            pltpu.SemaphoreType.DMA((3,)),
        ],
        compiler_params=pltpu.CompilerParams(
            collective_id=0, has_side_effects=True, vmem_limit_bytes=40 * 1024 * 1024
        ),
        name="exchange",
    )(series, lengths.reshape(1, pieces), starts.reshape(1, pieces))


def solution(mesh):
    placed = (P(("row", "col"), None), P(("row", "col")), P(("row", "col")))
    return jax.shard_map(
        on_device, mesh=mesh, in_specs=placed, out_specs=P("row", "col"), check_vma=False
    )
```

```python
import functools

import jax
import jax.numpy as jnp
from jax import lax
from jax.experimental import pallas as pl
from jax.experimental.pallas import tpu as pltpu
from jax.sharding import PartitionSpec as P

MESH = pl.DeviceIdType.MESH


def normalize(series, windows):
    count, steps = series.shape
    lane = lax.broadcasted_iota(jnp.int32, (count, 2 * count), 1)
    series_of = lax.broadcasted_iota(jnp.int32, (count, 2 * count), 0)
    spread = jnp.broadcast_to(windows[...], (count, 2 * count))

    def column(first_lane):
        return jnp.sum(jnp.where(lane == series_of + first_lane, spread, 0), axis=1, keepdims=True)

    valid, first = column(0), column(count)
    positions = lax.broadcasted_iota(jnp.int32, (count, steps), 1)
    inside = ((positions >= first) & (positions < first + valid)).astype(jnp.float32)
    valid_count = valid.astype(jnp.float32)
    average = jnp.sum(inside * series[...], axis=1, keepdims=True) / valid_count
    centered = inside * (series[...] - average)
    variance = jnp.sum(centered * centered, axis=1, keepdims=True) / valid_count
    return (centered / jnp.sqrt(valid_count * (variance + 1e-06))).astype(jnp.bfloat16)


PARTS = 2
COPIES = 140
SHORT = 1
FIRST = ["o", "x", "c"]
ORDER = (
    ("p", "l1", "l2.m", "h0", "h1", "f", "l2.e", "l3.m", "l3.e", "h2", "y", "q", "v", "h3")
    + ("A", "B", "w", "E", "C", "D")
)


def exchange(series_in, windows_in, out, *scratch):
    series, windows, own, rows, cols, passing = scratch[:6]
    send_sem, row_sem, col_sem, passing_sem, in_sem = scratch[6:]
    row, col = lax.axis_index("row"), lax.axis_index("col")
    half, y, core = row // 8, (row // 2) % 4, row % 2
    x, z = col // 4, col % 4
    right, left = (x + 1) % 4, (x + 3) % 4
    up, down = (y + 1) % 4, (y + 3) % 4

    def at_col(x_to, z_to):
        return (row, x_to * 4 + z_to)

    def at_y(y_to):
        return (half * 8 + y_to * 2 + core, col)

    sibling = (row + 1 - 2 * core, col)
    heights = [z, z + 1 - 2 * (z % 2), 2 - z // 2, 3 - 3 * (z // 2)]
    middle = z * (3 - z) // 2
    partner = at_col(x, heights[1])
    across = at_col(x, (3 - z) % 4)
    sides = [at_col(right, z), at_col(left, z)]
    ring = [at_y(up), at_y(down)]
    shift = 2 * (x % 2) + z // 2
    carrier = at_y((y + shift) % 4)
    moves = (shift + 3) // 4
    source = at_y((y + 4 - shift) % 4)
    theirs = half * 8 + ((y + 4 - shift) % 4) * 2 + core
    targets = [(h * 8 + y * 2 + 1 - z % 2, theirs) for h in (0, 1)]
    origin = (col // 2) % 4

    def places(y_of, height):
        turn = (y_of + 4 - origin) % 4
        near = turn // 2 * 4 + turn % 2 * 2 + height
        return near, near + 8

    carriers = [
        (col // 8 * 8 + y * 2 + col % 2, place) for place in places(y, 1 - core)
    ]

    loads = [
        pltpu.make_async_copy(src, dst, in_sem.at[i])
        for i, (src, dst) in enumerate(
            ((series_in, series), (windows_in, windows))
        )
    ]
    for load in loads:
        load.start()
    barrier = pltpu.get_barrier_semaphore()

    def greet(device):
        pl.semaphore_signal(barrier, inc=1, device_id=device, device_id_type=MESH)

    for device in [partner, sibling] + sides + ring + carriers:
        greet(device)
    pl.when(middle == 1)(functools.partial(greet, across))
    pl.when(moves == 1)(functools.partial(greet, source))
    for load in loads:
        load.wait()
    normed = normalize(series, windows)
    own[...] = normed
    rows[pl.ds(col * PARTS, PARTS)] = normed.reshape(PARTS, 64 // PARTS, own.shape[1])
    pl.semaphore_wait(barrier, 8 + middle + moves)

    sent = []

    def both(a, b):
        return b if a is None else a if b is None else a * b

    def send(src, dst, sem, device, when=None):
        copy = pltpu.make_async_remote_copy(
            src_ref=src,
            dst_ref=dst,
            send_sem=send_sem.at[len(sent)],
            recv_sem=sem,
            device_id=device,
            device_id_type=MESH,
        )
        if when is None:
            copy.start()
        else:
            pl.when(when == 1)(copy.start)
        sent.append((copy, when))

    def mine(part):
        return own.at[pl.ds(part * (64 // PARTS), 64 // PARTS)]

    def send_row(slot, part, device, src=None, when=None):
        i = slot * PARTS + part
        send(rows.at[i] if src is None else src, rows.at[i], row_sem.at[i], device, when)

    def send_col(slot, part, device, when=None):
        i = slot * PARTS + part
        send(cols.at[i], cols.at[i], col_sem.at[i], device, when)

    def wait(buffer, sem, i, when=None):
        copy = pltpu.make_async_remote_copy(
            src_ref=buffer.at[i],
            dst_ref=buffer.at[i],
            send_sem=send_sem.at[0],
            recv_sem=sem.at[i],
            device_id=sibling,
            device_id_type=MESH,
        )
        if when is None:
            copy.wait_recv()
        else:
            pl.when(when == 1)(copy.wait_recv)

    def wait_row(slot, part, when=None):
        wait(rows, row_sem, slot * PARTS + part, when)

    def wait_col(slot, part, when=None):
        wait(cols, col_sem, slot * PARTS + part, when)

    def carry(src, part, when):
        i = col * PARTS + part
        for target in targets:
            send(src, cols.at[i], col_sem.at[i], target, when)

    def start(name):
        for part in range(PARTS):
            if name == "x":
                for side in sides:
                    send_row(col, part, side, mine(part))
            elif name == "c":
                send(mine(part), passing.at[part], passing_sem.at[part], carrier, moves)
                carry(mine(part), part, 1 - moves)
            else:
                send_row(col, part, partner, mine(part))
                send_row(col, part, across, mine(part), middle)

    for name in FIRST:
        start(name)

    def step(name):
        kind, k = name[0], int(name[1:2].strip(".") or 0)
        on = None if "." not in name else middle if name[-1] == "m" else 1 - middle
        for part in range(PARTS):
            onward = part < PARTS // 2
            if kind == "l":
                slot = x * 4 + heights[k]
                wait_row(slot, part, on)
                if "e" not in name:
                    send_row(slot, part, across if k == 1 else partner, None, middle)
                one_way = k == 1 or (k == 2 and SHORT and "m" in name)
                for side in (sides[:1] if onward else sides[1:]) if one_way else sides:
                    send_row(slot, part, side, None, on)
            elif kind == "q":
                slot = (right if onward else left) * 4 + z
                wait_row(slot, part, on)
                send_row(slot, part, partner, None, on)
                if SHORT:
                    send_row(slot, part, across, None, middle if on is None or "m" in name else 0 * z)
            elif kind == "h":
                slot = (left if onward else right) * 4 + heights[k]
                wait_row(slot, part, on)
                send_row(slot, part, sides[0] if onward else sides[1], None, on)
            elif kind == "p":
                wait(passing, passing_sem, part, both(moves, on))
                carry(passing.at[part], part, both(moves, on))
            else:
                if kind == "f":
                    y_of, onto = y, ring
                elif kind == "y":
                    y_of, onto = (down, ring[:1]) if onward else (up, ring[1:])
                elif kind == "v":
                    y_of, onto = up if onward else down, []
                else:
                    y_of, onto = (y + 2) % 4, []
                for slot in places(y_of, 1 - core):
                    wait_col(slot, part, on)
                    for device in onto:
                        send_col(slot, part, device, on)
                    send_col(slot, part, sibling, on)

    steps = rows.shape[2]

    def tile(group, groups, *y_from):
        count = 4 * groups * PARTS
        left_rows = rows[pl.ds(group * 4 * PARTS, count)].reshape(groups * 256, steps)
        blocks = [place for y_of in y_from for place in places(y_of, 0)]
        right_rows = jnp.concatenate(
            [cols[pl.ds(place * PARTS, 2 * PARTS)].reshape(128, steps) for place in blocks], axis=0
        )
        block = lax.dot_general(
            left_rows, right_rows, (((1,), (1,)), ((), ())), preferred_element_type=jnp.float32
        )
        for k, place in enumerate(blocks):
            at = pl.multiple_of(place * 64, 128)
            out[pl.ds(group * 256, groups * 256), pl.ds(at, 128)] = block[:, k * 128 : k * 128 + 128]

    def wait_siblings(y_of):
        for slot in places(y_of, core):
            for part in range(PARTS):
                wait_col(slot, part)

    def loop(count, body):
        def run(i, carry):
            body(i)
            return carry

        lax.fori_loop(0, count, run, 0)

    def multiply(name):
        if name == "A":
            wait_siblings(y)
            tile(x, 1, y)
        elif name == "B":
            for height in heights[1:]:
                for part in range(PARTS):
                    wait_row((right if part < PARTS // 2 else left) * 4 + height, part)
            loop(2, lambda i: tile((x + 1 + 2 * i) % 4, 1, y))
        elif name == "E":
            wait_siblings(down)
            wait_siblings(up)
            loop(3, lambda i: tile((x + i + i // 2) % 4, 1, down, up))
        elif name == "C":
            for height in range(4):
                for part in range(PARTS):
                    wait_row((x + 2) % 4 * 4 + height, part)
            tile((x + 2) % 4, 1, y, down, up)
        else:
            wait_siblings((y + 2) % 4)
            tile(0, 4, (y + 2) % 4)

    for name in ORDER:
        if name.isupper():
            multiply(name)
        else:
            step(name)
    for copy, when in sent:
        if when is None:
            copy.wait_send()
        else:
            pl.when(when == 1)(copy.wait_send)


def on_device(series, lengths, starts):
    pieces, steps = series.shape
    windows = jnp.concatenate([lengths, starts]).reshape(1, 2 * pieces)
    part = pieces // PARTS
    shape = (16 * PARTS, part, steps)
    return pl.pallas_call(
        exchange,
        out_shape=jax.ShapeDtypeStruct((1024, 1024), jnp.float32),
        in_specs=[pl.BlockSpec(memory_space=pltpu.HBM)] * 2,
        out_specs=pl.BlockSpec(memory_space=pltpu.VMEM),
        scratch_shapes=[
            pltpu.VMEM((pieces, steps), jnp.float32),
            pltpu.VMEM((1, 2 * pieces), jnp.int32),
            pltpu.VMEM((pieces, steps), jnp.bfloat16),
            pltpu.VMEM(shape, jnp.bfloat16),
            pltpu.VMEM(shape, jnp.bfloat16),
            pltpu.VMEM((PARTS, part, steps), jnp.bfloat16),
            pltpu.SemaphoreType.DMA((COPIES,)),
            pltpu.SemaphoreType.DMA((16 * PARTS,)),
            pltpu.SemaphoreType.DMA((16 * PARTS,)),
            pltpu.SemaphoreType.DMA((PARTS,)),
            pltpu.SemaphoreType.DMA((2,)),
        ],
        compiler_params=pltpu.CompilerParams(
            collective_id=0, has_side_effects=True, vmem_limit_bytes=40 * 1024 * 1024
        ),
        name="exchange",
    )(series, windows)


def solution(mesh):
    placed = (P(("row", "col"), None), P(("row", "col")), P(("row", "col")))
    return jax.shard_map(
        on_device, mesh=mesh, in_specs=placed, out_specs=P("row", "col"), check_vma=False
    )
```

```python
import functools

import jax
import jax.numpy as jnp
from jax import lax
from jax.experimental import pallas as pl
from jax.experimental.pallas import tpu as pltpu
from jax.sharding import PartitionSpec as P

MESH = pl.DeviceIdType.MESH


def normalize(series, windows):
    count, steps = series.shape
    lane = lax.broadcasted_iota(jnp.int32, (count, 2 * count), 1)
    series_of = lax.broadcasted_iota(jnp.int32, (count, 2 * count), 0)
    spread = jnp.broadcast_to(windows[...], (count, 2 * count))

    def column(first_lane):
        return jnp.sum(jnp.where(lane == series_of + first_lane, spread, 0), axis=1, keepdims=True)

    valid, first = column(0), column(count)
    positions = lax.broadcasted_iota(jnp.int32, (count, steps), 1)
    inside = ((positions >= first) & (positions < first + valid)).astype(jnp.float32)
    valid_count = valid.astype(jnp.float32)
    average = jnp.sum(inside * series[...], axis=1, keepdims=True) / valid_count
    centered = inside * (series[...] - average)
    variance = jnp.sum(centered * centered, axis=1, keepdims=True) / valid_count
    return (centered / jnp.sqrt(valid_count * (variance + 1e-06))).astype(jnp.bfloat16)


PARTS = 2
COPIES = 140
FIRST = ["o", "x", "c"]
ORDER = (
    ("p", "l1", "l2.m", "h0", "h1", "f", "l2.e", "l3.m", "l3.e", "h2", "y", "q", "v", "h3")
    + ("A", "B", "w", "E", "C", "D")
)


def exchange(series_in, windows_in, out, *scratch):
    series, windows, own, rows, cols, passing = scratch[:6]
    send_sem, row_sem, col_sem, passing_sem, in_sem = scratch[6:]
    row, col = lax.axis_index("row"), lax.axis_index("col")
    half, y, core = row // 8, (row // 2) % 4, row % 2
    x, z = col // 4, col % 4
    right, left = (x + 1) % 4, (x + 3) % 4
    up, down = (y + 1) % 4, (y + 3) % 4

    def at_col(x_to, z_to):
        return (row, x_to * 4 + z_to)

    def at_y(y_to):
        return (half * 8 + y_to * 2 + core, col)

    sibling = (row + 1 - 2 * core, col)
    heights = [z, z + 1 - 2 * (z % 2), 2 - z // 2, 3 - 3 * (z // 2)]
    middle = z * (3 - z) // 2
    partner = at_col(x, heights[1])
    across = at_col(x, (3 - z) % 4)
    sides = [at_col(right, z), at_col(left, z)]
    ring = [at_y(up), at_y(down)]
    shift = 2 * (x % 2) + z // 2
    carrier = at_y((y + shift) % 4)
    moves = (shift + 3) // 4
    source = at_y((y + 4 - shift) % 4)
    theirs = half * 8 + ((y + 4 - shift) % 4) * 2 + core
    targets = [(h * 8 + y * 2 + 1 - z % 2, theirs) for h in (1 - half, half)]
    origin = (col // 2) % 4

    def places(y_of, height):
        turn = (y_of + 4 - origin) % 4
        near = turn // 2 * 4 + turn % 2 * 2 + height
        return near, near + 8

    carriers = [
        (col // 8 * 8 + y * 2 + col % 2, place) for place in places(y, 1 - core)
    ]

    loads = [
        pltpu.make_async_copy(src, dst, in_sem.at[i])
        for i, (src, dst) in enumerate(
            ((series_in, series), (windows_in, windows))
        )
    ]
    for load in loads:
        load.start()
    barrier = pltpu.get_barrier_semaphore()

    def greet(device):
        pl.semaphore_signal(barrier, inc=1, device_id=device, device_id_type=MESH)

    for device in [partner, sibling] + sides + ring + carriers:
        greet(device)
    pl.when(middle == 1)(functools.partial(greet, across))
    pl.when(moves == 1)(functools.partial(greet, source))
    for load in loads:
        load.wait()
    normed = normalize(series, windows)
    own[...] = normed
    rows[pl.ds(col * PARTS, PARTS)] = normed.reshape(PARTS, 64 // PARTS, own.shape[1])
    pl.semaphore_wait(barrier, 8 + middle + moves)

    sent = []

    def both(a, b):
        return b if a is None else a if b is None else a * b

    def send(src, dst, sem, device, when=None):
        copy = pltpu.make_async_remote_copy(
            src_ref=src,
            dst_ref=dst,
            send_sem=send_sem.at[len(sent)],
            recv_sem=sem,
            device_id=device,
            device_id_type=MESH,
        )
        if when is None:
            copy.start()
        else:
            pl.when(when == 1)(copy.start)
        sent.append((copy, when))

    def mine(part):
        return own.at[pl.ds(part * (64 // PARTS), 64 // PARTS)]

    def send_row(slot, part, device, src=None, when=None):
        i = slot * PARTS + part
        send(rows.at[i] if src is None else src, rows.at[i], row_sem.at[i], device, when)

    def send_col(slot, part, device, when=None):
        i = slot * PARTS + part
        send(cols.at[i], cols.at[i], col_sem.at[i], device, when)

    def wait(buffer, sem, i, when=None):
        copy = pltpu.make_async_remote_copy(
            src_ref=buffer.at[i],
            dst_ref=buffer.at[i],
            send_sem=send_sem.at[0],
            recv_sem=sem.at[i],
            device_id=sibling,
            device_id_type=MESH,
        )
        if when is None:
            copy.wait_recv()
        else:
            pl.when(when == 1)(copy.wait_recv)

    def wait_row(slot, part, when=None):
        wait(rows, row_sem, slot * PARTS + part, when)

    def wait_col(slot, part, when=None):
        wait(cols, col_sem, slot * PARTS + part, when)

    def carry(src, part, when):
        i = col * PARTS + part
        for target in targets:
            send(src, cols.at[i], col_sem.at[i], target, when)

    def start(name):
        for part in range(PARTS):
            if name == "x":
                for side in sides:
                    send_row(col, part, side, mine(part))
            elif name == "c":
                send(mine(part), passing.at[part], passing_sem.at[part], carrier, moves)
                carry(mine(part), part, 1 - moves)
            else:
                send_row(col, part, partner, mine(part))
                send_row(col, part, across, mine(part), middle)

    for name in FIRST:
        start(name)

    def step(name):
        kind, k = name[0], int(name[1:2].strip(".") or 0)
        on = None if "." not in name else middle if name[-1] == "m" else 1 - middle
        for part in range(PARTS):
            onward = part < PARTS // 2
            if kind == "l":
                slot = x * 4 + heights[k]
                wait_row(slot, part, on)
                if "e" not in name:
                    send_row(slot, part, across if k == 1 else partner, None, middle)
                one_way = k == 1
                for side in (sides[:1] if onward else sides[1:]) if one_way else sides:
                    send_row(slot, part, side, None, on)
            elif kind == "q":
                slot = (right if onward else left) * 4 + z
                wait_row(slot, part, on)
                send_row(slot, part, partner, None, on)
            elif kind == "h":
                slot = (left if onward else right) * 4 + heights[k]
                wait_row(slot, part, on)
                send_row(slot, part, sides[0] if onward else sides[1], None, on)
            elif kind == "p":
                wait(passing, passing_sem, part, both(moves, on))
                carry(passing.at[part], part, both(moves, on))
            else:
                if kind == "f":
                    y_of, onto = y, ring
                elif kind == "y":
                    y_of, onto = (down, ring[:1]) if onward else (up, ring[1:])
                elif kind == "v":
                    y_of, onto = up if onward else down, []
                else:
                    y_of, onto = (y + 2) % 4, []
                for slot in places(y_of, 1 - core):
                    wait_col(slot, part, on)
                    for device in onto:
                        send_col(slot, part, device, on)
                    send_col(slot, part, sibling, on)

    steps = rows.shape[2]

    def tile(group, groups, *y_from):
        count = 4 * groups * PARTS
        left_rows = rows[pl.ds(group * 4 * PARTS, count)].reshape(groups * 256, steps)
        blocks = [place for y_of in y_from for place in places(y_of, 0)]
        right_rows = jnp.concatenate(
            [cols[pl.ds(place * PARTS, 2 * PARTS)].reshape(128, steps) for place in blocks], axis=0
        )
        block = lax.dot_general(
            left_rows, right_rows, (((1,), (1,)), ((), ())), preferred_element_type=jnp.float32
        )
        for k, place in enumerate(blocks):
            at = pl.multiple_of(place * 64, 128)
            out[pl.ds(group * 256, groups * 256), pl.ds(at, 128)] = block[:, k * 128 : k * 128 + 128]

    def wait_siblings(y_of):
        for slot in places(y_of, core):
            for part in range(PARTS):
                wait_col(slot, part)

    def loop(count, body):
        def run(i, carry):
            body(i)
            return carry

        lax.fori_loop(0, count, run, 0)

    def multiply(name):
        if name == "A":
            wait_siblings(y)
            tile(x, 1, y)
        elif name == "B":
            for height in heights[1:]:
                for part in range(PARTS):
                    wait_row((right if part < PARTS // 2 else left) * 4 + height, part)
            loop(2, lambda i: tile((x + 1 + 2 * i) % 4, 1, y))
        elif name == "E":
            wait_siblings(down)
            wait_siblings(up)
            loop(3, lambda i: tile((x + i + i // 2) % 4, 1, down, up))
        elif name == "C":
            for height in range(4):
                for part in range(PARTS):
                    wait_row((x + 2) % 4 * 4 + height, part)
            tile((x + 2) % 4, 1, y, down, up)
        else:
            wait_siblings((y + 2) % 4)
            tile(0, 4, (y + 2) % 4)

    for name in ORDER:
        if name.isupper():
            multiply(name)
        else:
            step(name)
    for copy, when in sent:
        if when is None:
            copy.wait_send()
        else:
            pl.when(when == 1)(copy.wait_send)


def on_device(series, lengths, starts):
    pieces, steps = series.shape
    windows = jnp.concatenate([lengths, starts]).reshape(1, 2 * pieces)
    part = pieces // PARTS
    shape = (16 * PARTS, part, steps)
    return pl.pallas_call(
        exchange,
        out_shape=jax.ShapeDtypeStruct((1024, 1024), jnp.float32),
        in_specs=[pl.BlockSpec(memory_space=pltpu.HBM)] * 2,
        out_specs=pl.BlockSpec(memory_space=pltpu.VMEM),
        scratch_shapes=[
            pltpu.VMEM((pieces, steps), jnp.float32),
            pltpu.VMEM((1, 2 * pieces), jnp.int32),
            pltpu.VMEM((pieces, steps), jnp.bfloat16),
            pltpu.VMEM(shape, jnp.bfloat16),
            pltpu.VMEM(shape, jnp.bfloat16),
            pltpu.VMEM((PARTS, part, steps), jnp.bfloat16),
            pltpu.SemaphoreType.DMA((COPIES,)),
            pltpu.SemaphoreType.DMA((16 * PARTS,)),
            pltpu.SemaphoreType.DMA((16 * PARTS,)),
            pltpu.SemaphoreType.DMA((PARTS,)),
            pltpu.SemaphoreType.DMA((2,)),
        ],
        compiler_params=pltpu.CompilerParams(
            collective_id=0, has_side_effects=True, vmem_limit_bytes=40 * 1024 * 1024
        ),
        name="exchange",
    )(series, windows)


def solution(mesh):
    placed = (P(("row", "col"), None), P(("row", "col")), P(("row", "col")))
    return jax.shard_map(
        on_device, mesh=mesh, in_specs=placed, out_specs=P("row", "col"), check_vma=False
    )
```
